32 devices in a mesh: fit: 2 (over x), comp: 4 (over z), pts: 4 (over y, core).
Axes of the slice: x: 2, y: 2, z: 4, core: 2. Of those that a mesh axis runs over, the one named last changes fastest.
Arguments:
- points: bfloat16 [16384, 1024], P(('fit', 'pts')), parts along dimension 0
- means_init: float32 [32768, 1024], P(('fit', 'comp')), parts along dimension 0
- logw_init: float32 [32768], P(('fit', 'comp')), parts along dimension 0
- inv_temp: float32 [3], replicated
Outputs:
- output 1: float32 [32768, 1024], P(('fit', 'comp')), parts along dimension 0
- output 2: float32 [32768], P(('fit', 'comp')), parts along dimension 0
- output 3: float32 [16384], P(('fit', 'pts')), parts along dimension 0
There are 2 independent parts. The reference program is written for one: setup_inputs(seed, part) draws one part's arguments, and reference() takes and returns one part's arrays. A program takes and returns all parts, laid end to end along the dimension named above; an argument that names none is the same for every part.
All inputs are finite; a program needn't handle non-finite values.
Results may differ from the reference program's by a relative error of at most 0.001.
Values are sent between devices in bfloat16 or wider.
A program may use at most 1 GiB of HBM per device.

```python
import jax
import jax.numpy as jnp
from jax import lax

N = 8192
K = 16384
D = 1024
SWEEPS = 3
NUM_SRC = 16
ROW_BLOCK = 256

PRIOR_ALPHA = 1e-3
COUNT_EPS = 1e-6


def setup_inputs(seed: int = 0, part: int = 0) -> dict:
    root_key = jax.random.key(seed)
    part_key = jax.random.fold_in(root_key, part)
    key_cent, key_noise, key_assign, key_mnoise, key_logw = jax.random.split(part_key, 5)
    key_temp = jax.random.fold_in(root_key, 1000003)
    center_std = (2.0 / D ** 0.5) ** 0.5
    centers = center_std * jax.random.normal(key_cent, (NUM_SRC, D), jnp.float32)
    src_id = (jnp.arange(N, dtype=jnp.int32) * NUM_SRC) // N
    points = centers[src_id] + jax.random.normal(key_noise, (N, D), jnp.float32)
    assign = jax.random.randint(key_assign, (K,), 0, NUM_SRC)
    means_init = centers[assign] + 0.8 * jax.random.normal(key_mnoise, (K, D), jnp.float32)
    logw_init = jax.nn.log_softmax(0.5 * jax.random.normal(key_logw, (K,), jnp.float32))
    temp_steps = jax.random.uniform(key_temp, (SWEEPS,), jnp.float32)
    inv_temp = (0.25 + 0.2 * jnp.cumsum(temp_steps)) / D ** 0.5
    return {"points": points.astype(jnp.bfloat16), "means_init": means_init, "logw_init": logw_init, "inv_temp": inv_temp}


def em_sweep(points, mean_vecs, log_w, temp):
    mean_bf = mean_vecs.astype(jnp.bfloat16)
    mean_sq = jnp.sum(mean_vecs * mean_vecs, axis=1)
    row_blocks = points.reshape(N // ROW_BLOCK, ROW_BLOCK, D)

    def scan_body(state_pair, row_blk):
        counts, stat_sums = state_pair
        x_sq = jnp.sum(jnp.square(row_blk.astype(jnp.float32)), axis=1)
        cross_dot = jnp.dot(row_blk, mean_bf.T, preferred_element_type=jnp.float32)
        logits = log_w[None, :] - temp * (x_sq[:, None] - 2.0 * cross_dot + mean_sq[None, :])
        row_top = jnp.max(logits, axis=1)
        exp_total = jnp.sum(jnp.exp(logits - row_top[:, None]), axis=1)
        log_norm = row_top + jnp.log(exp_total)
        resp_prob = jnp.exp(logits - log_norm[:, None])
        counts = counts + jnp.sum(resp_prob, axis=0)
        stat_sums = stat_sums + jnp.dot(resp_prob.astype(jnp.bfloat16).T, row_blk, preferred_element_type=jnp.float32)
        return (counts, stat_sums), log_norm

    init_state = (jnp.zeros((K,), jnp.float32), jnp.zeros((K, D), jnp.float32))
    (counts, stat_sums), log_norm = lax.scan(scan_body, init_state, row_blocks)
    new_means = stat_sums / (counts[:, None] + COUNT_EPS)
    new_logw = jnp.log((counts + PRIOR_ALPHA) / (N + K * PRIOR_ALPHA))
    return new_means, new_logw, log_norm.reshape(N)


def reference(points, means_init, logw_init, inv_temp):
    mean_vecs = means_init
    log_w = logw_init
    log_norm = jnp.zeros((N,), jnp.float32)
    for sweep_idx in range(SWEEPS):
        mean_vecs, log_w, log_norm = em_sweep(points, mean_vecs, log_w, inv_temp[sweep_idx])
    return mean_vecs, log_w, log_norm
```

```python
import jax
import jax.numpy as jnp
from jax import lax
from jax.experimental import pallas as pl
from jax.experimental.pallas import tpu as pltpu
from jax.sharding import PartitionSpec as P

PRIOR_ALPHA = 1e-3
COUNT_EPS = 1e-6
F32, BF16 = jnp.float32, jnp.bfloat16
MESH = pl.DeviceIdType.MESH

NB = 1024
STRIP = NB // 2
PIECE = 128
CH = 256


def flip(p, a):
    y = lax.rem(p // 2 + a // 2, 2)
    c = lax.rem(lax.rem(p, 2) + lax.rem(a, 2), 2)
    return 2 * y + c


def em_kernel(beta, x_in, mu_in, lw_in, q_in, mu_out, n_out, lse_out, xg,
              pm, xbuf, mub, ab0, ab1, rb0, rb1, S, nacc, hmu_b, lw_b, mst, sst, qv, lse,
              own1, buf1, own2, buf2,
              fsem, xsem, qsend, qrecv, s1s, s1r, s2s, s2r,
              sib_s, sib_r, py_s, py_r, pz_s, pz_r, fw_s, fw_r, osem):
    kd, d = S.shape
    nblk = pm.shape[0]
    sweeps = beta.shape[0]
    z, p = lax.axis_index("comp"), lax.axis_index("pts")
    half = lax.rem(z, 2)
    zpair = z + 1 - 2 * half
    p1, p2 = flip(p, 1), flip(p, 2)

    barrier = pltpu.get_barrier_semaphore()
    for a in (1, 2, 3):
        pl.semaphore_signal(barrier, inc=1, device_id={"comp": lax.rem(z + a, 4)}, device_id_type=MESH)
        pl.semaphore_signal(barrier, inc=1, device_id={"pts": flip(p, a)}, device_id_type=MESH)
    pl.semaphore_wait(barrier, 6)

    def remote(src, dst, ss, rs, **dev):
        return pltpu.make_async_remote_copy(src_ref=src, dst_ref=dst, send_sem=ss, recv_sem=rs, device_id=dev, device_id_type=MESH)

    def rows(o, hf, i):
        return pl.ds(pl.multiple_of(o * 2048 + hf * 1024 + i * PIECE, PIECE), PIECE)

    own_rows = pl.ds(pl.multiple_of(p * 2048, 2048), 2048)
    sib = remote(x_in, xg.at[own_rows], sib_s, sib_r, pts=p1)
    py = lambda i: remote(x_in.at[pl.ds(pl.multiple_of(half * 1024 + i * PIECE, PIECE), PIECE)], xg.at[rows(p, half, i)], py_s.at[i], py_r.at[i], pts=p2)
    pz = lambda i: remote(xg.at[rows(p2, half, i)], xg.at[rows(p2, half, i)], pz_s.at[i], pz_r.at[i], comp=zpair)
    fwa = lambda i: remote(xg.at[rows(p2, half, i)], xg.at[rows(p2, half, i)], fw_s.at[i], fw_r.at[i], pts=p1)
    fwb = lambda i: remote(xg.at[rows(p2, 1 - half, i)], xg.at[rows(p2, 1 - half, i)], fw_s.at[8 + i], fw_r.at[8 + i], pts=p1)
    for i in range(8):
        py(i).start()
    qrow = lambda o: pl.ds(2 * o, 2)
    qcp = [remote(q_in, qv.at[qrow(p)], qsend.at[a - 1], qrecv.at[a - 1], pts=flip(p, a)) for a in (1, 2, 3)]
    for c in qcp:
        c.start()
    sib.start()
    st = [pltpu.make_async_copy(x_in.at[pl.ds(i * 1024, 1024)], (rb0, rb1)[i], xsem.at[i]) for i in range(2)]
    for c in st:
        c.start()
    mcp = pltpu.make_async_copy(mu_in.at[pl.ds(pl.multiple_of(p * kd, kd), kd)], S, osem)
    mcp.start()
    qv[qrow(p)] = q_in[...]
    lw_b[...] = lw_in[...]
    for i, c in enumerate(st):
        c.wait()
        st[i] = pltpu.make_async_copy((rb0, rb1)[i], xg.at[pl.ds(pl.multiple_of(p * 2048 + i * 1024, 1024), 1024)], xsem.at[i])
        st[i].start()
    mcp.wait()
    for c in st:
        c.wait()
    for c in qcp:
        c.wait()

    def take_py(i):
        py(i).wait_recv()
        pz(i).start()
        fwa(i).start()

    def take_pz(i):
        pz(i).wait_recv()
        fwb(i).start()

    def arrive(n):
        if n == 2:
            sib.wait_recv()
        elif n == 4:
            take_py(0)
            for i in range(1, 5):
                take_py(i)
                take_pz(i - 1)
        elif n == 6:
            for i in range(5, 8):
                take_py(i)
                take_pz(i - 1)
            take_pz(7)
        elif n in (5, 7):
            for i in range(4):
                fwa(i + 4 * (n == 7)).wait_recv()
                fwb(i + 4 * (n == 7)).wait_recv()

    def fetch(b, slot):
        o, h = b // 2, lax.rem(b, 2)
        return [pltpu.make_async_copy(xg.at[pl.ds(pl.multiple_of(o * 2048 + g * 1024 + h * STRIP, STRIP), STRIP)],
                                      xbuf.at[slot, pl.ds(g * STRIP, STRIP)], fsem.at[slot, g]) for g in range(2)]

    def start(cs):
        for c in cs:
            c.start()

    def wait(cs):
        for c in cs:
            c.wait()

    def sweep(t, _):
        par = lax.rem(t, 2)
        first_sweep = t == 0
        pe = jnp.where(first_sweep, p, 0)
        nb2 = -2.0 * beta[t]

        def order(k):
            r = 2 * (k // 4) + jnp.where(first_sweep, lax.rem(k, 2) * (k // 4) + (lax.rem(k, 4) // 2) * (1 - k // 4), lax.rem(k, 4) // 2)
            h = jnp.where(first_sweep, lax.rem(k, 2) * (1 - k // 4) + (lax.rem(k, 4) // 2) * (k // 4), lax.rem(k, 2))
            return 2 * flip(pe, r) + h

        start(fetch(order(0), 0))
        mub[...] = S[...].astype(BF16)
        hmu_b[...] = jnp.broadcast_to(0.5 * jnp.sum(S[...] * S[...], axis=1, keepdims=True), hmu_b.shape)
        nacc[...] = jnp.zeros_like(nacc)

        def send1(k):
            return [remote(own1.at[k], buf1.at[a - 1, k], s1s.at[a - 1, k], s1r.at[a - 1, k], comp=lax.rem(z + a, 4)) for a in (1, 2, 3)]

        def send2(b):
            return [remote(own2.at[b], buf2.at[par, a - 1, b], s2s.at[a - 1, b], s2r.at[par, a - 1, b], pts=flip(p, a)) for a in (1, 2, 3)]

        def merge(ms):
            m, s = [v[0:1] for v in ms], [v[1:2] for v in ms]
            top = jnp.maximum(jnp.maximum(m[0], m[1]), jnp.maximum(m[2], m[3]))
            return top, sum(si * jnp.exp(mi - top) for mi, si in zip(m, s))

        def publish(k):
            b = order(k)
            mm = jnp.max(mst[b], axis=0, keepdims=True)
            own1[k, 0:1] = mm
            own1[k, 1:2] = jnp.sum(sst[b] * jnp.exp(mst[b] - mm), axis=0, keepdims=True)
            start(send1(k))

        def relay(k):
            wait(send1(k))
            b = order(k)
            mm, ss = merge([own1[k]] + [buf1[a, k] for a in range(3)])
            own2[b, 0:1] = mm
            own2[b, 1:2] = ss
            start(send2(b))

        def settle(b):
            wait(send2(b))
            mm, ss = merge([own2[b]] + [buf2[par, a, b] for a in range(3)])
            l = mm + jnp.log(ss)
            lse[b] = l
            mst[b] = jnp.exp(mst[b] - l)

        def step_a(k, dst, src, slot, first, last, prepare):
            if not last:
                wait(fetch(order(k), slot))
                for cond, n in prepare:
                    @pl.when(jnp.logical_and(first_sweep, cond))
                    def _():
                        arrive(n)
                if prepare:
                    start(fetch(order(k + 1), 1 - slot))
            if not first:
                b = order(k - 1)
            for u in range(NB // 256):
                sl = slice(u * 256, (u + 1) * 256)
                if not last:
                    dst[:, sl] = lax.dot_general(mub[...], xbuf[slot, sl, :], (((1,), (1,)), ((), ())), preferred_element_type=F32)
                if not first:
                    for l0 in (u * 256, u * 256 + 128):
                        ln = slice(l0, l0 + 128)
                        q = jnp.broadcast_to(qv[b, :, ln], (CH, 128))
                        for c in range(kd // CH):
                            r = slice(c * CH, (c + 1) * CH)
                            lg = lw_b[r, :] + nb2 * ((hmu_b[r, :] - src[r, ln]) + q)
                            m = jnp.max(lg, axis=0, keepdims=True)
                            e = jnp.exp(lg - m)
                            pm[b, r, ln] = e
                            mst[b, c:c + 1, ln] = m
                            sst[b, c:c + 1, ln] = jnp.sum(e, axis=0, keepdims=True)
            if not first:
                publish(k - 1)

        yes = t >= 0
        step_a(0, ab0, ab1, 0, True, False, [(yes, 1)])

        def body_a(i, _):
            step_a(2 * i + 1, ab1, ab0, 1, False, False, [(i == 0, 2), (i == 1, 4), (i == 2, 6)])

            @pl.when(i > 0)
            def _():
                relay(2 * i - 2)
                relay(2 * i - 1)
            step_a(2 * i + 2, ab0, ab1, 0, False, False, [(i == 1, 5), (i == 2, 7)])
            return 0

        lax.fori_loop(0, nblk // 2 - 1, body_a, 0)
        step_a(nblk - 1, ab1, ab0, 1, False, False, [])
        start(fetch(0, 0))
        relay(nblk - 4)
        relay(nblk - 3)
        step_a(nblk, ab0, ab1, 0, False, True, [])
        relay(nblk - 2)
        relay(nblk - 1)

        S[...] = jnp.zeros_like(S)

        def step_s(j, rd, rs, slot, first, last):
            if not last:
                settle(j)
            if not first:
                wait(fetch(j - 1, slot))
                if not last:
                    start(fetch(j, 1 - slot))
            for u in range(4):
                if not last:
                    for r0 in range(u * (kd // 4), (u + 1) * (kd // 4), 16):
                        r = slice(r0, r0 + 16)
                        c = r0 // CH
                        rr = pm[j, r, :] * jnp.broadcast_to(mst[j, c:c + 1, :], (16, NB))
                        rd[r, :] = rr.astype(BF16)
                        acc = rr[:, 0:128]
                        for l0 in range(128, NB, 128):
                            acc += rr[:, l0:l0 + 128]
                        nacc[r, :] += acc
                if not first:
                    sl = slice(u * (d // 4), (u + 1) * (d // 4))
                    S[:, sl] += jnp.dot(rs[...], xbuf[slot, :, sl], preferred_element_type=F32)

        step_s(0, rb0, rb1, 1, True, False)

        def body_s(i, _):
            step_s(2 * i + 1, rb1, rb0, 0, False, False)
            step_s(2 * i + 2, rb0, rb1, 1, False, False)
            return 0

        lax.fori_loop(0, nblk // 2 - 1, body_s, 0)
        step_s(nblk - 1, rb1, rb0, 0, False, False)
        step_s(nblk, rb0, rb1, 1, False, True)
        n = jnp.sum(nacc[...], axis=1, keepdims=True)
        S[...] = S[...] * (1.0 / (n + COUNT_EPS))
        lw = jnp.log((n + PRIOR_ALPHA) / (nblk * NB + 16 * kd * PRIOR_ALPHA))
        lw_b[...] = jnp.broadcast_to(lw, lw_b.shape)
        return 0

    lax.fori_loop(0, sweeps, sweep, 0)

    sib.wait_send()
    for i in range(8):
        py(i).wait_send()
        pz(i).wait_send()
        fwa(i).wait_send()
        fwb(i).wait_send()
    ocp = pltpu.make_async_copy(S, mu_out, osem)
    ocp.start()
    n_out[...] = lw_b[...]
    lse_out[...] = lse[qrow(p)]
    ocp.wait()


def solution(mesh):
    def per_device(points, mean_vecs, log_w, inv_temp):
        n_loc, d = points.shape
        k_loc = mean_vecs.shape[0]
        kd = k_loc // mesh.shape["pts"]
        nblk = n_loc * mesh.shape["pts"] // NB
        p = lax.axis_index("pts")
        x_sq = 0.5 * jnp.sum(jnp.square(points.astype(F32)), axis=1)
        q_in = x_sq.reshape(2, 2, STRIP).transpose(1, 0, 2).reshape(2, 1, NB)
        lw_in = jnp.broadcast_to(lax.dynamic_slice(log_w, (p * kd,), (kd,))[:, None], (kd, 128))
        V, D = pltpu.VMEM, pltpu.SemaphoreType.DMA
        bs = lambda m: pl.BlockSpec(memory_space=m)
        mu, lw_b, lse, _ = pl.pallas_call(
            em_kernel,
            out_shape=(
                jax.ShapeDtypeStruct((kd, d), F32),
                jax.ShapeDtypeStruct((kd, 128), F32),
                jax.ShapeDtypeStruct((2, 1, NB), F32),
                jax.ShapeDtypeStruct((nblk * NB, d), BF16),
            ),
            in_specs=[bs(pltpu.SMEM), bs(pl.ANY), bs(pl.ANY), bs(V), bs(V)],
            out_specs=(bs(pl.ANY), bs(V), bs(V), bs(pl.ANY)),
            scratch_shapes=[
                V((nblk, kd, NB), F32), V((2, NB, d), BF16), V((kd, d), BF16),
                V((kd, NB), F32), V((kd, NB), F32), V((kd, NB), BF16), V((kd, NB), BF16),
                V((kd, d), F32), V((kd, 128), F32), V((kd, 128), F32), V((kd, 128), F32),
                V((nblk, kd // CH, NB), F32), V((nblk, kd // CH, NB), F32),
                V((nblk, 1, NB), F32), V((nblk, 1, NB), F32),
                V((nblk, 2, NB), F32), V((3, nblk, 2, NB), F32),
                V((nblk, 2, NB), F32), V((2, 3, nblk, 2, NB), F32),
                D((2, 2)), D((2,)), D((3,)), D((3,)),
                D((3, nblk)), D((3, nblk)), D((3, nblk)), D((2, 3, nblk)),
                D, D, D((8,)), D((8,)), D((8,)), D((8,)), D((16,)), D((16,)), D,
            ],
            compiler_params=pltpu.CompilerParams(
                collective_id=0, has_side_effects=True, vmem_limit_bytes=67043328),
            name="em_sweeps",
        )(inv_temp, points, mean_vecs, lw_in, q_in)
        means = lax.all_gather(mu, "pts", axis=0, tiled=True)
        logw = lax.all_gather(lw_b[:, 0], "pts", axis=0, tiled=True)
        lse_rows = lse.reshape(2, 2, STRIP).transpose(1, 0, 2).reshape(n_loc)
        return means, logw, lse_rows

    comp_spec, row_spec = P(("fit", "comp")), P(("fit", "pts"))
    return jax.shard_map(
        per_device,
        mesh=mesh,
        in_specs=(P(("fit", "pts"), None), P(("fit", "comp"), None), comp_spec, P()),
        out_specs=(P(("fit", "comp"), None), comp_spec, row_spec),
        check_vma=False,
    )
```

```python
import jax
import jax.numpy as jnp
from jax import lax
from jax.experimental import pallas as pl
from jax.experimental.pallas import tpu as pltpu
from jax.sharding import PartitionSpec as P

PRIOR_ALPHA = 1e-3
COUNT_EPS = 1e-6
F32, BF16 = jnp.float32, jnp.bfloat16
MESH = pl.DeviceIdType.MESH

NB = 1024
STRIP = NB // 2
PIECE = 128
FAR = 384
CH = 256


def flip(p, a):
    y = lax.rem(p // 2 + a // 2, 2)
    c = lax.rem(lax.rem(p, 2) + lax.rem(a, 2), 2)
    return 2 * y + c


def em_kernel(beta, x_in, mu_in, lw_in, q_in, mu_out, lw_out, lse_out, xg,
              pm, xbuf, mub, ab0, ab1, rb0, rb1, S, nacc, hmu_b, lw_b, mst, sst, qv, lse,
              own1, buf1, own2, buf2, mub2, hmu_b2, lw_b2, row1, row2, lw_all,
              fsem, xsem, qsend, qrecv, s1s, s1r, s2s, s2r,
              sib_s, sib_r, py_s, py_r, pz_s, pz_r, fw_s, fw_r,
              b_s, b_r, w_s, w_r, o_s, o_r, osem):
    kd, d = S.shape
    nblk = pm.shape[0]
    sweeps = beta.shape[0]
    z, p = lax.axis_index("comp"), lax.axis_index("pts")
    half = lax.rem(z, 2)
    zpair = z + 1 - 2 * half
    p1, p2 = flip(p, 1), flip(p, 2)

    barrier = pltpu.get_barrier_semaphore()
    for a in (1, 2, 3):
        pl.semaphore_signal(barrier, inc=1, device_id={"comp": lax.rem(z + a, 4)}, device_id_type=MESH)
        pl.semaphore_signal(barrier, inc=1, device_id={"pts": flip(p, a)}, device_id_type=MESH)
    pl.semaphore_wait(barrier, 6)

    def remote(src, dst, ss, rs, **dev):
        return pltpu.make_async_remote_copy(src_ref=src, dst_ref=dst, send_sem=ss, recv_sem=rs, device_id=dev, device_id_type=MESH)

    def rows(o, hf, i):
        return pl.ds(pl.multiple_of(o * 2048 + hf * 1024 + i * PIECE, PIECE), PIECE)

    own_rows = pl.ds(pl.multiple_of(p * 2048, 2048), 2048)
    sib = remote(x_in, xg.at[own_rows], sib_s, sib_r, pts=p1)
    py = lambda i: remote(x_in.at[pl.ds(pl.multiple_of(half * 1024 + i * PIECE, PIECE), PIECE)], xg.at[rows(p, half, i)], py_s.at[i], py_r.at[i], pts=p2)
    pz = lambda i: remote(xg.at[rows(p2, half, i)], xg.at[rows(p2, half, i)], pz_s.at[i], pz_r.at[i], comp=zpair)
    fwa = lambda i: remote(xg.at[rows(p2, half, i)], xg.at[rows(p2, half, i)], fw_s.at[i], fw_r.at[i], pts=p1)
    fwb = lambda i: remote(xg.at[rows(p2, 1 - half, i)], xg.at[rows(p2, 1 - half, i)], fw_s.at[8 + i], fw_r.at[8 + i], pts=p1)
    qrow = lambda o: pl.ds(2 * o, 2)
    qcp = [remote(q_in, qv.at[qrow(p)], qsend.at[a - 1], qrecv.at[a - 1], pts=flip(p, a)) for a in (1, 2, 3)]
    for c in qcp:
        c.start()
    for i in range(8):
        py(i).start()
    sib.start()
    st = [pltpu.make_async_copy(x_in.at[pl.ds(i * 1024, 1024)], (rb0, rb1)[i], xsem.at[i]) for i in range(2)]
    for c in st:
        c.start()
    mcp = pltpu.make_async_copy(mu_in.at[pl.ds(pl.multiple_of(p * kd, kd), kd)], S, osem.at[0])
    mcp.start()
    lcp = pltpu.make_async_copy(lw_in, lw_b, osem.at[1])
    lcp.start()
    qv[qrow(p)] = q_in[...]
    for i, c in enumerate(st):
        c.wait()
        st[i] = pltpu.make_async_copy((rb0, rb1)[i], xg.at[pl.ds(pl.multiple_of(p * 2048 + i * 1024, 1024), 1024)], xsem.at[i])
        st[i].start()
    mcp.wait()
    lcp.wait()
    for c in st:
        c.wait()
    for c in qcp:
        c.wait()

    rest = pl.ds(FAR, kd - FAR)
    mid = (kd - FAR) // 2
    bulk = lambda i: remote(mub.at[pl.ds(FAR + i * mid, mid)], mub2.at[pl.ds(i * mid, mid)], b_s.at[i], b_r.at[i], pts=p2)
    bulk_rows = lambda: remote(row1, row2, b_s.at[2], b_r.at[2], pts=p2)

    def as_row(ref, g):
        blk = ref[g * 128:(g + 1) * 128, :]
        eye = lax.broadcasted_iota(jnp.int32, (128, 128), 0) == lax.broadcasted_iota(jnp.int32, (128, 128), 1)
        return jnp.sum(jnp.where(eye, blk, 0.0), axis=0, keepdims=True)

    def take_py(i):
        py(i).wait_recv()
        pz(i).start()
        fwa(i).start()

    def take_pz(i):
        pz(i).wait_recv()
        fwb(i).start()

    def arrive(n):
        if n == 2:
            sib.wait_recv()
        elif n == 4:
            take_py(0)
            for i in range(1, 5):
                take_py(i)
                take_pz(i - 1)
        elif n == 6:
            for i in range(5, 8):
                take_py(i)
                take_pz(i - 1)
            take_pz(7)
        elif n in (5, 7):
            for i in range(4):
                fwa(i + 4 * (n == 7)).wait_recv()
                fwb(i + 4 * (n == 7)).wait_recv()

    def fetch(b, slot):
        o, h = b // 2, lax.rem(b, 2)
        return [pltpu.make_async_copy(xg.at[pl.ds(pl.multiple_of(o * 2048 + g * 1024 + h * STRIP, STRIP), STRIP)],
                                      xbuf.at[slot, pl.ds(g * STRIP, STRIP)], fsem.at[slot, g]) for g in range(2)]

    def start(cs):
        for c in cs:
            c.start()

    def wait(cs):
        for c in cs:
            c.wait()

    def sweep(t, _):
        par = lax.rem(t, 2)
        first_sweep = t == 0
        pe = jnp.where(first_sweep, p, 0)
        nb2 = -2.0 * beta[t]

        def order(k):
            r = 2 * (k // 4) + jnp.where(first_sweep, lax.rem(k, 2) * (k // 4) + (lax.rem(k, 4) // 2) * (1 - k // 4), lax.rem(k, 4) // 2)
            h = jnp.where(first_sweep, lax.rem(k, 2) * (1 - k // 4) + (lax.rem(k, 4) // 2) * (k // 4), lax.rem(k, 2))
            return 2 * flip(pe, r) + h

        start(fetch(order(0), 0))
        def load_means(g, _):
            r = pl.ds(pl.multiple_of(g * 64, 64), 64)
            v = S[r, :]
            mub[r, :] = v.astype(BF16)
            hmu_b[r, :] = jnp.broadcast_to(0.5 * jnp.sum(v * v, axis=1, keepdims=True), (64, 128))
            nacc[r, :] = jnp.zeros((64, 128), F32)
            return 0

        lax.fori_loop(0, kd // 64, load_means, 0)

        @pl.when(t == sweeps - 1)
        def _():
            for g in range(kd // 128):
                row1[0, g:g + 1, :] = as_row(hmu_b, g)
                row1[1, g:g + 1, :] = as_row(lw_b, g)
            bulk_rows().start()
            bulk(0).start()

        def send1(k):
            return [remote(own1.at[k], buf1.at[a - 1, k], s1s.at[a - 1, k], s1r.at[a - 1, k], comp=lax.rem(z + a, 4)) for a in (1, 2, 3)]

        def send2(b):
            return [remote(own2.at[b], buf2.at[par, a - 1, b], s2s.at[a - 1, b], s2r.at[par, a - 1, b], pts=flip(p, a)) for a in (1, 2, 3)]

        def merge(ms):
            m, s = [v[0:1] for v in ms], [v[1:2] for v in ms]
            top = jnp.maximum(jnp.maximum(m[0], m[1]), jnp.maximum(m[2], m[3]))
            return top, sum(si * jnp.exp(mi - top) for mi, si in zip(m, s))

        def publish(k):
            b = order(k)
            mm = jnp.max(mst[b], axis=0, keepdims=True)
            own1[k, 0:1] = mm
            own1[k, 1:2] = jnp.sum(sst[b] * jnp.exp(mst[b] - mm), axis=0, keepdims=True)
            start(send1(k))

        def relay(k):
            wait(send1(k))
            b = order(k)
            mm, ss = merge([own1[k]] + [buf1[a, k] for a in range(3)])
            own2[b, 0:1] = mm
            own2[b, 1:2] = ss
            start(send2(b))

        def settle(b):
            wait(send2(b))
            mm, ss = merge([own2[b]] + [buf2[par, a, b] for a in range(3)])
            l = mm + jnp.log(ss)
            lse[b] = l
            mst[b] = jnp.exp(mst[b] - l)

        def step_a(k, dst, src, slot, first, last, prepare):
            if not last:
                wait(fetch(order(k), slot))
                for cond, n in prepare:
                    @pl.when(jnp.logical_and(first_sweep, cond))
                    def _():
                        arrive(n)
                if prepare:
                    start(fetch(order(k + 1), 1 - slot))
            if not first:
                b = order(k - 1)
            for u in range(NB // 256):
                sl = slice(u * 256, (u + 1) * 256)
                if not last:
                    dst[:, sl] = lax.dot_general(mub[...], xbuf[slot, sl, :], (((1,), (1,)), ((), ())), preferred_element_type=F32)
                if not first:
                    for l0 in (u * 256, u * 256 + 128):
                        ln = slice(l0, l0 + 128)
                        q = jnp.broadcast_to(qv[b, :, ln], (CH, 128))
                        for c in range(kd // CH):
                            r = slice(c * CH, (c + 1) * CH)
                            lg = lw_b[r, :] + nb2 * ((hmu_b[r, :] - src[r, ln]) + q)
                            m = jnp.max(lg, axis=0, keepdims=True)
                            e = jnp.exp(lg - m)
                            pm[b, r, ln] = e
                            mst[b, c:c + 1, ln] = m
                            sst[b, c:c + 1, ln] = jnp.sum(e, axis=0, keepdims=True)
            if not first:
                publish(k - 1)

        yes = t >= 0
        step_a(0, ab0, ab1, 0, True, False, [(yes, 1)])

        def body_a(i, _):
            step_a(2 * i + 1, ab1, ab0, 1, False, False, [(i == 0, 2), (i == 1, 4), (i == 2, 6)])

            @pl.when(i > 0)
            def _():
                relay(2 * i - 2)
                relay(2 * i - 1)
            step_a(2 * i + 2, ab0, ab1, 0, False, False, [(i == 1, 5), (i == 2, 7)])
            return 0

        lax.fori_loop(0, nblk // 2 - 1, body_a, 0)
        step_a(nblk - 1, ab1, ab0, 1, False, False, [])
        start(fetch(0, 0))
        relay(nblk - 4)
        relay(nblk - 3)
        step_a(nblk, ab0, ab1, 0, False, True, [])
        relay(nblk - 2)

        @pl.when(first_sweep)
        def _():
            relay(nblk - 1)

        S[...] = jnp.zeros_like(S)

        def step_s(j, rd, rs, slot, first, last):
            if not last:
                settle(j)
            if not first:
                wait(fetch(j - 1, slot))
                if not last:
                    start(fetch(j, 1 - slot))
            for u in range(4):
                if not last:
                    for r0 in range(u * (kd // 4), (u + 1) * (kd // 4), 16):
                        r = slice(r0, r0 + 16)
                        c = r0 // CH
                        rr = pm[j, r, :] * jnp.broadcast_to(mst[j, c:c + 1, :], (16, NB))
                        rd[r, :] = rr.astype(BF16)
                        acc = rr[:, 0:128]
                        for l0 in range(128, NB, 128):
                            acc += rr[:, l0:l0 + 128]
                        nacc[r, :] += acc
                if not first:
                    sl = slice(u * (d // 4), (u + 1) * (d // 4))
                    S[:, sl] += jnp.dot(rs[...], xbuf[slot, :, sl], preferred_element_type=F32)

        step_s(0, rb0, rb1, 1, True, False)

        def body_s(i, _):
            step_s(2 * i + 1, rb1, rb0, 0, False, False)

            @pl.when(jnp.logical_and(i == 0, t > 0))
            def _():
                relay(nblk - 1)

            @pl.when(jnp.logical_and(i == 0, t == sweeps - 1))
            def _():
                bulk(1).start()
            step_s(2 * i + 2, rb0, rb1, 1, False, False)
            return 0

        lax.fori_loop(0, nblk // 2 - 1, body_s, 0)
        step_s(nblk - 1, rb1, rb0, 0, False, False)
        step_s(nblk, rb0, rb1, 1, False, True)
        def finish(g, _):
            r = pl.ds(pl.multiple_of(g * 64, 64), 64)
            n = jnp.sum(nacc[r, :], axis=1, keepdims=True)
            S[r, :] = S[r, :] * (1.0 / (n + COUNT_EPS))
            lw = jnp.log((n + PRIOR_ALPHA) / (nblk * NB + 16 * kd * PRIOR_ALPHA))
            lw_b[r, :] = jnp.broadcast_to(lw, (64, 128))
            return 0

        lax.fori_loop(0, kd // 64, finish, 0)
        return 0

    lax.fori_loop(0, sweeps, sweep, 0)

    quarter = lambda o, r0, n: pl.ds(pl.multiple_of(o * kd + r0, 128), n)
    out_own = pltpu.make_async_copy(S, mu_out.at[quarter(p, 0, kd)], osem.at[0])
    out_sib = remote(S, mu_out.at[quarter(p, 0, kd)], o_s.at[0], o_r.at[0], pts=p1)
    out_far = [remote(S.at[pl.ds(i * 128, 128)], mu_out.at[quarter(p, i * 128, 128)], o_s.at[1 + i], o_r.at[1 + i], pts=p2) for i in range(FAR // 128)]
    out_fwd = [remote(mu_out.at[quarter(p2, i * 128, 128)], mu_out.at[quarter(p2, i * 128, 128)], o_s.at[4 + i], o_r.at[4 + i], pts=p1) for i in range(FAR // 128)]
    for g in range(kd // 128):
        lw_all[p, g:g + 1, :] = as_row(lw_b, g)
    out_lw = [remote(lw_all.at[p], lw_all.at[p], w_s.at[a - 1], w_r.at[a - 1], pts=flip(p, a)) for a in (1, 2, 3)]
    start(out_lw)
    start(out_far)
    out_own.start()
    out_sib.start()

    rn = kd - FAR
    S2 = pm.at[0]
    bulk_rows().wait()
    for i in range(2):
        bulk(i).wait()
    for g in range(rn // 128):
        for v, ref in ((0, hmu_b2), (1, lw_b2)):
            ref[g * 128:(g + 1) * 128, :] = jnp.broadcast_to(row2[v, FAR // 128 + g:FAR // 128 + g + 1, :], (128, 128)).T
    nb2 = -2.0 * beta[sweeps - 1]
    nacc[...] = jnp.zeros_like(nacc)
    S2[0:rn, :] = jnp.zeros((rn, d), F32)
    start(fetch(0, 0))

    def step_d(j, dst, src, rb, first, last):
        now, before = lax.rem(j, 3), lax.rem(j + 2, 3)
        if not last:
            wait(fetch(j, now))

            @pl.when(j + 1 < nblk)
            def _():
                start(fetch(j + 1, lax.rem(j + 1, 3)))
        for u in range(4):
            if not last:
                sl = slice(u * (NB // 4), (u + 1) * (NB // 4))
                dst[0:rn, sl] = lax.dot_general(mub2[...], xbuf[now, sl, :], (((1,), (1,)), ((), ())), preferred_element_type=F32)
            if not first:
                for r0 in range(u * (rn // 4), (u + 1) * (rn // 4), 16):
                    r = slice(r0, r0 + 16)
                    wide = lambda ref: jnp.concatenate([ref[r, :]] * (NB // 128), axis=1)
                    spread = lambda v: jnp.broadcast_to(v, (16, NB))
                    lg = wide(lw_b2) + nb2 * ((wide(hmu_b2) - src[r, :]) + spread(qv[j - 1]))
                    rr = jnp.exp(lg - spread(lse[j - 1]))
                    rb[r, :] = rr.astype(BF16)
                    acc = rr[:, 0:128]
                    for l0 in range(128, NB, 128):
                        acc += rr[:, l0:l0 + 128]
                    nacc[r, :] += acc
        if not first:
            for u in range(4):
                sl = slice(u * (d // 4), (u + 1) * (d // 4))
                S2[0:rn, sl] += jnp.dot(rb[0:rn, :], xbuf[before, :, sl], preferred_element_type=F32)

    step_d(0, ab0, ab1, rb0, True, False)

    def body_d(i, _):
        step_d(2 * i + 1, ab1, ab0, rb0, False, False)
        step_d(2 * i + 2, ab0, ab1, rb1, False, False)
        return 0

    lax.fori_loop(0, nblk // 2 - 1, body_d, 0)
    step_d(nblk - 1, ab1, ab0, rb0, False, False)
    step_d(nblk, ab0, ab1, rb1, False, True)

    def finish2(g, _):
        r = pl.ds(pl.multiple_of(g * 64, 64), 64)
        n2 = jnp.sum(nacc[r, :], axis=1, keepdims=True)
        S2[r, :] = S2[r, :] * (1.0 / (n2 + COUNT_EPS))
        return 0

    lax.fori_loop(0, rn // 64, finish2, 0)
    src2 = S2.at[pl.ds(0, rn)]
    out_dup = pltpu.make_async_copy(src2, mu_out.at[quarter(p2, FAR, rn)], osem.at[1])
    out_dsib = remote(src2, mu_out.at[quarter(p2, FAR, rn)], o_s.at[7], o_r.at[7], pts=p1)
    out_dsib.start()
    out_dup.start()
    for c, f in zip(out_far, out_fwd):
        c.wait()
        f.start()
    sib.wait_send()
    for i in range(8):
        py(i).wait_send()
        pz(i).wait_send()
        fwa(i).wait_send()
        fwb(i).wait_send()
    wait(out_lw)
    lw_out[...] = lw_all[...]
    lse_out[...] = lse[qrow(p)]
    out_own.wait()
    out_sib.wait()
    wait(out_fwd)
    out_dup.wait()
    out_dsib.wait()


def solution(mesh):
    def per_device(points, mean_vecs, log_w, inv_temp):
        n_loc, d = points.shape
        k_loc = mean_vecs.shape[0]
        kd = k_loc // mesh.shape["pts"]
        nblk = n_loc * mesh.shape["pts"] // NB
        p = lax.axis_index("pts")
        x_sq = 0.5 * jnp.sum(jnp.square(points.astype(F32)), axis=1)
        q_in = x_sq.reshape(2, 2, STRIP).transpose(1, 0, 2).reshape(2, 1, NB)
        lw_in = jnp.broadcast_to(lax.dynamic_slice(log_w, (p * kd,), (kd,))[:, None], (kd, 128))
        V, D = pltpu.VMEM, pltpu.SemaphoreType.DMA
        bs = lambda m: pl.BlockSpec(memory_space=m)
        means, logw, lse, _ = pl.pallas_call(
            em_kernel,
            out_shape=(
                jax.ShapeDtypeStruct((k_loc, d), F32),
                jax.ShapeDtypeStruct((k_loc // kd, kd // 128, 128), F32),
                jax.ShapeDtypeStruct((2, 1, NB), F32),
                jax.ShapeDtypeStruct((nblk * NB, d), BF16),
            ),
            in_specs=[bs(pltpu.SMEM), bs(pl.ANY), bs(pl.ANY), bs(pl.ANY), bs(V)],
            out_specs=(bs(pl.ANY), bs(V), bs(V), bs(pl.ANY)),
            scratch_shapes=[
                V((nblk, kd, NB), F32), V((3, NB, d), BF16), V((kd, d), BF16),
                V((kd, NB), F32), V((kd, NB), F32), V((kd, NB), BF16), V((kd, NB), BF16),
                V((kd, d), F32), V((kd, 128), F32), V((kd, 128), F32), V((kd, 128), F32),
                V((nblk, kd // CH, NB), F32), V((nblk, kd // CH, NB), F32),
                V((nblk, 1, NB), F32), V((nblk, 1, NB), F32),
                V((nblk, 2, NB), F32), V((3, nblk, 2, NB), F32),
                V((nblk, 2, NB), F32), V((2, 3, nblk, 2, NB), F32),
                V((kd - FAR, d), BF16), V((kd - FAR, 128), F32), V((kd - FAR, 128), F32),
                V((2, kd // 128, 128), F32), V((2, kd // 128, 128), F32), V((k_loc // kd, kd // 128, 128), F32),
                D((3, 2)), D((2,)), D((3,)), D((3,)),
                D((3, nblk)), D((3, nblk)), D((3, nblk)), D((2, 3, nblk)),
                D, D, D((8,)), D((8,)), D((8,)), D((8,)), D((16,)), D((16,)),
                D((3,)), D((3,)), D((3,)), D((3,)), D((8,)), D((8,)), D((2,)),
            ],
            compiler_params=pltpu.CompilerParams(
                collective_id=0, has_side_effects=True, vmem_limit_bytes=67043328),
            name="em_sweeps",
        )(inv_temp, points, mean_vecs, lw_in, q_in)
        lse_rows = lse.reshape(2, 2, STRIP).transpose(1, 0, 2).reshape(n_loc)
        return means, logw.reshape(k_loc), lse_rows

    comp_spec, row_spec = P(("fit", "comp")), P(("fit", "pts"))
    return jax.shard_map(
        per_device,
        mesh=mesh,
        in_specs=(P(("fit", "pts"), None), P(("fit", "comp"), None), comp_spec, P()),
        out_specs=(P(("fit", "comp"), None), comp_spec, row_spec),
        check_vma=False,
    )
```

```python
import jax
import jax.numpy as jnp
from jax import lax
from jax.experimental import pallas as pl
from jax.experimental.pallas import tpu as pltpu
from jax.sharding import PartitionSpec as P

PRIOR_ALPHA = 1e-3
COUNT_EPS = 1e-6
F32, BF16 = jnp.float32, jnp.bfloat16
MESH = pl.DeviceIdType.MESH

NB = 1024
STRIP = NB // 2
PIECE = 128
FAR = 256
CH = 256


def flip(p, a):
    y = lax.rem(p // 2 + a // 2, 2)
    c = lax.rem(lax.rem(p, 2) + lax.rem(a, 2), 2)
    return 2 * y + c


def em_kernel(beta, x_in, mu_in, lw_in, q_in, mu_out, lw_out, lse_out, xg,
              pm, xbuf, mub, ab0, ab1, rb0, rb1, S, nacc, hmu_b, lw_b, mst, sst, qv, lse,
              own1, buf1, own2, buf2, mub2, hmu_b2, lw_b2, row1, row2, lw_all,
              fsem, xsem, qsend, qrecv, s1s, s1r, s2s, s2r,
              sib_s, sib_r, py_s, py_r, pz_s, pz_r, fw_s, fw_r,
              b_s, b_r, w_s, w_r, o_s, o_r, osem):
    kd, d = S.shape
    nblk = pm.shape[0]
    sweeps = beta.shape[0]
    z, p = lax.axis_index("comp"), lax.axis_index("pts")
    half = lax.rem(z, 2)
    zpair = z + 1 - 2 * half
    p1, p2 = flip(p, 1), flip(p, 2)

    barrier = pltpu.get_barrier_semaphore()
    for a in (1, 2, 3):
        pl.semaphore_signal(barrier, inc=1, device_id={"comp": lax.rem(z + a, 4)}, device_id_type=MESH)
        pl.semaphore_signal(barrier, inc=1, device_id={"pts": flip(p, a)}, device_id_type=MESH)
    pl.semaphore_wait(barrier, 6)

    def remote(src, dst, ss, rs, **dev):
        return pltpu.make_async_remote_copy(src_ref=src, dst_ref=dst, send_sem=ss, recv_sem=rs, device_id=dev, device_id_type=MESH)

    def rows(o, hf, i):
        return pl.ds(pl.multiple_of(o * 2048 + hf * 1024 + i * PIECE, PIECE), PIECE)

    own_rows = pl.ds(pl.multiple_of(p * 2048, 2048), 2048)
    sib = remote(x_in, xg.at[own_rows], sib_s, sib_r, pts=p1)
    py = lambda i: remote(x_in.at[pl.ds(pl.multiple_of(half * 1024 + i * PIECE, PIECE), PIECE)], xg.at[rows(p, half, i)], py_s.at[i], py_r.at[i], pts=p2)
    pz = lambda i: remote(xg.at[rows(p2, half, i)], xg.at[rows(p2, half, i)], pz_s.at[i], pz_r.at[i], comp=zpair)
    fwa = lambda i: remote(xg.at[rows(p2, half, i)], xg.at[rows(p2, half, i)], fw_s.at[i], fw_r.at[i], pts=p1)
    fwb = lambda i: remote(xg.at[rows(p2, 1 - half, i)], xg.at[rows(p2, 1 - half, i)], fw_s.at[8 + i], fw_r.at[8 + i], pts=p1)
    qrow = lambda o: pl.ds(2 * o, 2)
    qcp = [remote(q_in, qv.at[qrow(p)], qsend.at[a - 1], qrecv.at[a - 1], pts=flip(p, a)) for a in (1, 2, 3)]
    for c in qcp:
        c.start()
    for i in range(8):
        py(i).start()
    sib.start()
    st = [pltpu.make_async_copy(x_in.at[pl.ds(i * 1024, 1024)], (rb0, rb1)[i], xsem.at[i]) for i in range(2)]
    for c in st:
        c.start()
    mcp = pltpu.make_async_copy(mu_in.at[pl.ds(pl.multiple_of(p * kd, kd), kd)], S, osem.at[0])
    mcp.start()
    lcp = pltpu.make_async_copy(lw_in, lw_b, osem.at[1])
    lcp.start()
    qv[qrow(p)] = q_in[...]
    for i, c in enumerate(st):
        c.wait()
        st[i] = pltpu.make_async_copy((rb0, rb1)[i], xg.at[pl.ds(pl.multiple_of(p * 2048 + i * 1024, 1024), 1024)], xsem.at[i])
        st[i].start()
    mcp.wait()
    lcp.wait()
    for c in st:
        c.wait()
    for c in qcp:
        c.wait()

    rest = pl.ds(FAR, kd - FAR)
    mid = (kd - FAR) // 2
    bulk = lambda i: remote(mub.at[pl.ds(FAR + i * mid, mid)], mub2.at[pl.ds(i * mid, mid)], b_s.at[i], b_r.at[i], pts=p2)
    bulk_rows = lambda: remote(row1, row2, b_s.at[2], b_r.at[2], pts=p2)

    def as_row(ref, g):
        blk = ref[g * 128:(g + 1) * 128, :]
        eye = lax.broadcasted_iota(jnp.int32, (128, 128), 0) == lax.broadcasted_iota(jnp.int32, (128, 128), 1)
        return jnp.sum(jnp.where(eye, blk, 0.0), axis=0, keepdims=True)

    def take_py(i):
        py(i).wait_recv()
        pz(i).start()
        fwa(i).start()

    def take_pz(i):
        pz(i).wait_recv()
        fwb(i).start()

    def arrive(n):
        if n == 1:
            sib.wait_recv()
        elif n == 4:
            take_py(0)
            for i in range(1, 5):
                take_py(i)
                take_pz(i - 1)
        elif n == 6:
            take_py(7)
            take_pz(6)
            take_pz(7)
        elif n in (5, 7):
            for i in range(4):
                fwa(i + 4 * (n == 7)).wait_recv()
                fwb(i + 4 * (n == 7)).wait_recv()

    def fetch(b, slot):
        o, h = b // 2, lax.rem(b, 2)
        return [pltpu.make_async_copy(xg.at[pl.ds(pl.multiple_of(o * 2048 + g * 1024 + h * STRIP, STRIP), STRIP)],
                                      xbuf.at[slot, pl.ds(g * STRIP, STRIP)], fsem.at[slot, g]) for g in range(2)]

    def start(cs):
        for c in cs:
            c.start()

    def wait(cs):
        for c in cs:
            c.wait()

    def sweep(t, _):
        par = lax.rem(t, 2)
        first_sweep = t == 0
        pe = jnp.where(first_sweep, p, 0)
        nb2 = -2.0 * beta[t]

        def order_s(j):
            return 2 * lax.rem(j, 4) + j // 4

        def order(k):
            r = jnp.where(first_sweep, 2 * (k // 4) + lax.rem(k, 2), lax.rem(k, 4))
            h = jnp.where(first_sweep, lax.rem(k, 4) // 2, k // 4)
            return 2 * flip(pe, r) + h

        start(fetch(order(0), 0))
        def load_means(g, _):
            r = pl.ds(pl.multiple_of(g * 64, 64), 64)
            v = S[r, :]
            mub[r, :] = v.astype(BF16)
            hmu_b[r, :] = jnp.broadcast_to(0.5 * jnp.sum(v * v, axis=1, keepdims=True), (64, 128))
            nacc[r, :] = jnp.zeros((64, 128), F32)
            return 0

        lax.fori_loop(0, kd // 64, load_means, 0)

        @pl.when(t == sweeps - 1)
        def _():
            for g in range(kd // 128):
                row1[0, g:g + 1, :] = as_row(hmu_b, g)
                row1[1, g:g + 1, :] = as_row(lw_b, g)
            bulk_rows().start()
            bulk(0).start()

        def send1(k):
            return [remote(own1.at[k], buf1.at[a - 1, k], s1s.at[a - 1, k], s1r.at[a - 1, k], comp=lax.rem(z + a, 4)) for a in (1, 2, 3)]

        def send2(b):
            return [remote(own2.at[b], buf2.at[par, a - 1, b], s2s.at[a - 1, b], s2r.at[par, a - 1, b], pts=flip(p, a)) for a in (1, 2, 3)]

        def merge(ms):
            m, s = [v[0:1] for v in ms], [v[1:2] for v in ms]
            top = jnp.maximum(jnp.maximum(m[0], m[1]), jnp.maximum(m[2], m[3]))
            return top, sum(si * jnp.exp(mi - top) for mi, si in zip(m, s))

        def publish(k):
            b = order(k)
            mm = jnp.max(mst[b], axis=0, keepdims=True)
            own1[k, 0:1] = mm
            own1[k, 1:2] = jnp.sum(sst[b] * jnp.exp(mst[b] - mm), axis=0, keepdims=True)
            start(send1(k))

        def relay(k):
            wait(send1(k))
            b = order(k)
            mm, ss = merge([own1[k]] + [buf1[a, k] for a in range(3)])
            own2[b, 0:1] = mm
            own2[b, 1:2] = ss
            start(send2(b))

        def settle(b):
            wait(send2(b))
            mm, ss = merge([own2[b]] + [buf2[par, a, b] for a in range(3)])
            l = mm + jnp.log(ss)
            lse[b] = l
            mst[b] = jnp.exp(mst[b] - l)

        def step_a(k, dst, src, slot, first, last, prepare=(), nxt=None):
            if not last:
                wait(fetch(order(k), slot))
                for cond, n in prepare:
                    @pl.when(jnp.logical_and(first_sweep, cond))
                    def _():
                        arrive(n)
                if nxt is not None:
                    start(fetch(nxt, 1 - slot))
            if not first:
                b = order(k - 1)
            for u in range(NB // 256):
                sl = slice(u * 256, (u + 1) * 256)
                if not last:
                    dst[:, sl] = lax.dot_general(mub[...], xbuf[slot, sl, :], (((1,), (1,)), ((), ())), preferred_element_type=F32)
                if not first:
                    for l0 in (u * 256, u * 256 + 128):
                        ln = slice(l0, l0 + 128)
                        q = jnp.broadcast_to(qv[b, :, ln], (CH, 128))
                        for c in range(kd // CH):
                            r = slice(c * CH, (c + 1) * CH)
                            lg = lw_b[r, :] + nb2 * ((hmu_b[r, :] - src[r, ln]) + q)
                            m = jnp.max(lg, axis=0, keepdims=True)
                            e = jnp.exp(lg - m)
                            pm[b, r, ln] = e
                            mst[b, c:c + 1, ln] = m
                            sst[b, c:c + 1, ln] = jnp.sum(e, axis=0, keepdims=True)
            if not first:
                publish(k - 1)

        def rounds_a(g, a0, na, s0):
            @pl.when(g == 1)
            def _():
                arrive(6)
                start(fetch(order(a0), 0))
            step_a(a0, ab0, ab1, 0, True, False, [(g == 0, 1), (g == 1, 7)], order(a0 + 1))

            def pair_a(i):
                k = a0 + 2 * i + 1
                more = 2 * i + 2 < na
                step_a(k, ab1, ab0, 1, False, False, [(k == 3, 4)], jnp.where(more, order(k + 1), order_s(s0)))

                @pl.when(i > 0)
                def _():
                    relay(k - 3)
                    relay(k - 2)

                @pl.when(more)
                def _():
                    step_a(k + 1, ab0, ab1, 0, False, False, [(k == 3, 5)], order(k + 2))

                @pl.when(jnp.logical_not(more))
                def _():
                    step_a(k + 1, ab0, ab1, 0, False, True)

            def body_a(i, _):
                @pl.when(2 * i + 1 < na)
                def _():
                    pair_a(i)
                return 0

            lax.fori_loop(0, nblk // 2, body_a, 0)
            relay(a0 + na - 2)

            @pl.when(first_sweep)
            def _():
                relay(a0 + na - 1)

        def step_s(place, rd, rs, slot, first, last):
            j = order_s(place)
            if not last:
                settle(j)
            if not first:
                wait(fetch(j, slot))
                if not last:
                    start(fetch(j, 1 - slot))
            for u in range(4):
                if not last:
                    for r0 in range(u * (kd // 4), (u + 1) * (kd // 4), 16):
                        r = slice(r0, r0 + 16)
                        c = r0 // CH
                        rr = pm[j, r, :] * jnp.broadcast_to(mst[j, c:c + 1, :], (16, NB))
                        rd[r, :] = rr.astype(BF16)
                        acc = rr[:, 0:128]
                        for l0 in range(128, NB, 128):
                            acc += rr[:, l0:l0 + 128]
                        nacc[r, :] += acc
                if not first:
                    sl = slice(u * (d // 4), (u + 1) * (d // 4))
                    S[:, sl] += jnp.dot(rs[...], xbuf[slot, :, sl], preferred_element_type=F32)

        def rounds(g):
            a0, s0 = 6 * g, 4 * g
            na = jnp.where(first_sweep, 6 - 4 * g, nblk)
            ns = jnp.where(first_sweep, nblk // 2, nblk)
            rounds_a(g, a0, na, s0)

            @pl.when(g == 0)
            def _():
                S[...] = jnp.zeros_like(S)
            step_s(s0, rb0, rb1, 1, True, False)

            def pair_s(i):
                j = s0 + 2 * i + 1
                more = 2 * i + 2 < ns
                step_s(j, rb1, rb0, 0, False, False)

                @pl.when(jnp.logical_and(i == 0, t > 0))
                def _():
                    relay(nblk - 1)

                @pl.when(jnp.logical_and(i == 0, t == sweeps - 1))
                def _():
                    bulk(1).start()

                for v in (0, 1):
                    @pl.when(jnp.logical_and(jnp.logical_and(first_sweep, g == 0), i == v))
                    def _():
                        take_py(5 + v)
                        take_pz(4 + v)

                @pl.when(more)
                def _():
                    step_s(j + 1, rb0, rb1, 1, False, False)

                @pl.when(jnp.logical_not(more))
                def _():
                    step_s(j + 1, rb0, rb1, 1, False, True)

            def body_s(i, _):
                @pl.when(2 * i + 1 < ns)
                def _():
                    pair_s(i)
                return 0

            lax.fori_loop(0, nblk // 2, body_s, 0)

        def body_r(g, _):
            @pl.when(jnp.logical_or(first_sweep, g == 0))
            def _():
                rounds(g)
            return 0

        lax.fori_loop(0, 2, body_r, 0)

        def finish(g, _):
            r = pl.ds(pl.multiple_of(g * 64, 64), 64)
            n = jnp.sum(nacc[r, :], axis=1, keepdims=True)
            S[r, :] = S[r, :] * (1.0 / (n + COUNT_EPS))
            lw = jnp.log((n + PRIOR_ALPHA) / (nblk * NB + 16 * kd * PRIOR_ALPHA))
            lw_b[r, :] = jnp.broadcast_to(lw, (64, 128))
            return 0

        lax.fori_loop(0, kd // 64, finish, 0)
        return 0

    lax.fori_loop(0, sweeps, sweep, 0)

    quarter = lambda o, r0, n: pl.ds(pl.multiple_of(o * kd + r0, 128), n)
    out_own = pltpu.make_async_copy(S, mu_out.at[quarter(p, 0, kd)], osem.at[0])
    out_sib = remote(S, mu_out.at[quarter(p, 0, kd)], o_s.at[0], o_r.at[0], pts=p1)
    out_far = [remote(S.at[pl.ds(i * 128, 128)], mu_out.at[quarter(p, i * 128, 128)], o_s.at[1 + i], o_r.at[1 + i], pts=p2) for i in range(FAR // 128)]
    out_fwd = [remote(mu_out.at[quarter(p2, i * 128, 128)], mu_out.at[quarter(p2, i * 128, 128)], o_s.at[4 + i], o_r.at[4 + i], pts=p1) for i in range(FAR // 128)]
    for g in range(kd // 128):
        lw_all[p, g:g + 1, :] = as_row(lw_b, g)
    out_lw = [remote(lw_all.at[p], lw_all.at[p], w_s.at[a - 1], w_r.at[a - 1], pts=flip(p, a)) for a in (1, 2, 3)]
    start(out_lw)
    start(out_far)
    out_own.start()
    out_sib.start()

    rn = kd - FAR
    S2 = pm.at[0]
    bulk_rows().wait()
    for i in range(2):
        bulk(i).wait()
    for g in range(rn // 128):
        for v, ref in ((0, hmu_b2), (1, lw_b2)):
            ref[g * 128:(g + 1) * 128, :] = jnp.broadcast_to(row2[v, FAR // 128 + g:FAR // 128 + g + 1, :], (128, 128)).T
    nb2 = -2.0 * beta[sweeps - 1]
    nacc[...] = jnp.zeros_like(nacc)
    S2[0:rn, :] = jnp.zeros((rn, d), F32)
    start(fetch(0, 0))

    def step_d(j, dst, src, rb, first, last):
        now, before = lax.rem(j, 3), lax.rem(j + 2, 3)
        if not last:
            wait(fetch(j, now))

            @pl.when(j + 1 < nblk)
            def _():
                start(fetch(j + 1, lax.rem(j + 1, 3)))
        for u in range(4):
            if not last:
                sl = slice(u * (NB // 4), (u + 1) * (NB // 4))
                dst[0:rn, sl] = lax.dot_general(mub2[...], xbuf[now, sl, :], (((1,), (1,)), ((), ())), preferred_element_type=F32)
            if not first:
                for r0 in range(u * (rn // 4), (u + 1) * (rn // 4), 16):
                    r = slice(r0, r0 + 16)
                    wide = lambda ref: jnp.concatenate([ref[r, :]] * (NB // 128), axis=1)
                    spread = lambda v: jnp.broadcast_to(v, (16, NB))
                    lg = wide(lw_b2) + nb2 * ((wide(hmu_b2) - src[r, :]) + spread(qv[j - 1]))
                    rr = jnp.exp(lg - spread(lse[j - 1]))
                    rb[r, :] = rr.astype(BF16)
                    acc = rr[:, 0:128]
                    for l0 in range(128, NB, 128):
                        acc += rr[:, l0:l0 + 128]
                    nacc[r, :] += acc
        if not first:
            for u in range(4):
                sl = slice(u * (d // 4), (u + 1) * (d // 4))
                S2[0:rn, sl] += jnp.dot(rb[0:rn, :], xbuf[before, :, sl], preferred_element_type=F32)

    step_d(0, ab0, ab1, rb0, True, False)

    def body_d(i, _):
        step_d(2 * i + 1, ab1, ab0, rb0, False, False)
        step_d(2 * i + 2, ab0, ab1, rb1, False, False)
        return 0

    lax.fori_loop(0, nblk // 2 - 1, body_d, 0)
    step_d(nblk - 1, ab1, ab0, rb0, False, False)
    step_d(nblk, ab0, ab1, rb1, False, True)

    def finish2(g, _):
        r = pl.ds(pl.multiple_of(g * 64, 64), 64)
        n2 = jnp.sum(nacc[r, :], axis=1, keepdims=True)
        S2[r, :] = S2[r, :] * (1.0 / (n2 + COUNT_EPS))
        return 0

    lax.fori_loop(0, rn // 64, finish2, 0)
    src2 = S2.at[pl.ds(0, rn)]
    out_dup = pltpu.make_async_copy(src2, mu_out.at[quarter(p2, FAR, rn)], osem.at[1])
    out_dsib = remote(src2, mu_out.at[quarter(p2, FAR, rn)], o_s.at[7], o_r.at[7], pts=p1)
    out_dsib.start()
    out_dup.start()
    for c, f in zip(out_far, out_fwd):
        c.wait()
        f.start()
    sib.wait_send()
    for i in range(8):
        py(i).wait_send()
        pz(i).wait_send()
        fwa(i).wait_send()
        fwb(i).wait_send()
    wait(out_lw)
    lw_out[...] = lw_all[...]
    lse_out[...] = lse[qrow(p)]
    out_own.wait()
    out_sib.wait()
    wait(out_fwd)
    out_dup.wait()
    out_dsib.wait()


def solution(mesh):
    def per_device(points, mean_vecs, log_w, inv_temp):
        n_loc, d = points.shape
        k_loc = mean_vecs.shape[0]
        kd = k_loc // mesh.shape["pts"]
        nblk = n_loc * mesh.shape["pts"] // NB
        p = lax.axis_index("pts")
        x_sq = 0.5 * jnp.sum(jnp.square(points.astype(F32)), axis=1)
        q_in = x_sq.reshape(2, 2, STRIP).transpose(1, 0, 2).reshape(2, 1, NB)
        lw_in = jnp.broadcast_to(lax.dynamic_slice(log_w, (p * kd,), (kd,))[:, None], (kd, 128))
        V, D = pltpu.VMEM, pltpu.SemaphoreType.DMA
        bs = lambda m: pl.BlockSpec(memory_space=m)
        means, logw, lse, _ = pl.pallas_call(
            em_kernel,
            out_shape=(
                jax.ShapeDtypeStruct((k_loc, d), F32),
                jax.ShapeDtypeStruct((k_loc // kd, kd // 128, 128), F32),
                jax.ShapeDtypeStruct((2, 1, NB), F32),
                jax.ShapeDtypeStruct((nblk * NB, d), BF16),
            ),
            in_specs=[bs(pltpu.SMEM), bs(pl.ANY), bs(pl.ANY), bs(pl.ANY), bs(V)],
            out_specs=(bs(pl.ANY), bs(V), bs(V), bs(pl.ANY)),
            scratch_shapes=[
                V((nblk, kd, NB), F32), V((3, NB, d), BF16), V((kd, d), BF16),
                V((kd, NB), F32), V((kd, NB), F32), V((kd, NB), BF16), V((kd, NB), BF16),
                V((kd, d), F32), V((kd, 128), F32), V((kd, 128), F32), V((kd, 128), F32),
                V((nblk, kd // CH, NB), F32), V((nblk, kd // CH, NB), F32),
                V((nblk, 1, NB), F32), V((nblk, 1, NB), F32),
                V((nblk, 2, NB), F32), V((3, nblk, 2, NB), F32),
                V((nblk, 2, NB), F32), V((2, 3, nblk, 2, NB), F32),
                V((kd - FAR, d), BF16), V((kd - FAR, 128), F32), V((kd - FAR, 128), F32),
                V((2, kd // 128, 128), F32), V((2, kd // 128, 128), F32), V((k_loc // kd, kd // 128, 128), F32),
                D((3, 2)), D((2,)), D((3,)), D((3,)),
                D((3, nblk)), D((3, nblk)), D((3, nblk)), D((2, 3, nblk)),
                D, D, D((8,)), D((8,)), D((8,)), D((8,)), D((16,)), D((16,)),
                D((3,)), D((3,)), D((3,)), D((3,)), D((8,)), D((8,)), D((2,)),
            ],
            compiler_params=pltpu.CompilerParams(
                collective_id=0, has_side_effects=True, vmem_limit_bytes=67043328),
            name="em_sweeps",
        )(inv_temp, points, mean_vecs, lw_in, q_in)
        lse_rows = lse.reshape(2, 2, STRIP).transpose(1, 0, 2).reshape(n_loc)
        return means, logw.reshape(k_loc), lse_rows

    comp_spec, row_spec = P(("fit", "comp")), P(("fit", "pts"))
    return jax.shard_map(
        per_device,
        mesh=mesh,
        in_specs=(P(("fit", "pts"), None), P(("fit", "comp"), None), comp_spec, P()),
        out_specs=(P(("fit", "comp"), None), comp_spec, row_spec),
        check_vma=False,
    )
```

```python
import jax
import jax.numpy as jnp
from jax import lax
from jax.experimental import pallas as pl
from jax.experimental.pallas import tpu as pltpu
from jax.sharding import PartitionSpec as P

PRIOR_ALPHA = 1e-3
COUNT_EPS = 1e-6
F32, BF16 = jnp.float32, jnp.bfloat16
MESH = pl.DeviceIdType.MESH

NB = 1024
STRIP = NB // 2
PIECE = 128
FAR = 384
CH = 256


def flip(p, a):
    y = lax.rem(p // 2 + a // 2, 2)
    c = lax.rem(lax.rem(p, 2) + lax.rem(a, 2), 2)
    return 2 * y + c


def em_kernel(beta, x_in, mu_in, lw_in, q_in, mu_out, lw_out, lse_out, xg,
              pm, xbuf, mub, ab0, ab1, rb0, rb1, S, nacc, hmu_b, lw_b, mst, sst, qv, lse,
              own1, buf1, own2, buf2, mub2, hmu_b2, lw_b2, row1, row2, lw_all,
              fsem, xsem, qsend, qrecv, s1s, s1r, s2s, s2r,
              sib_s, sib_r, py_s, py_r, pz_s, pz_r, fw_s, fw_r,
              b_s, b_r, w_s, w_r, o_s, o_r, osem):
    kd, d = S.shape
    nblk = pm.shape[0]
    sweeps = beta.shape[0]
    z, p = lax.axis_index("comp"), lax.axis_index("pts")
    half = lax.rem(z, 2)
    zpair = z + 1 - 2 * half
    p1, p2 = flip(p, 1), flip(p, 2)

    barrier = pltpu.get_barrier_semaphore()
    for a in (1, 2, 3):
        pl.semaphore_signal(barrier, inc=1, device_id={"comp": lax.rem(z + a, 4)}, device_id_type=MESH)
        pl.semaphore_signal(barrier, inc=1, device_id={"pts": flip(p, a)}, device_id_type=MESH)
    pl.semaphore_wait(barrier, 6)

    def remote(src, dst, ss, rs, **dev):
        return pltpu.make_async_remote_copy(src_ref=src, dst_ref=dst, send_sem=ss, recv_sem=rs, device_id=dev, device_id_type=MESH)

    def rows(o, hf, i):
        return pl.ds(pl.multiple_of(o * 2048 + hf * 1024 + i * PIECE, PIECE), PIECE)

    own_rows = pl.ds(pl.multiple_of(p * 2048, 2048), 2048)
    sib = remote(x_in, xg.at[own_rows], sib_s, sib_r, pts=p1)
    py = lambda i: remote(x_in.at[pl.ds(pl.multiple_of(half * 1024 + i * PIECE, PIECE), PIECE)], xg.at[rows(p, half, i)], py_s.at[i], py_r.at[i], pts=p2)
    pz = lambda i: remote(xg.at[rows(p2, half, i)], xg.at[rows(p2, half, i)], pz_s.at[i], pz_r.at[i], comp=zpair)
    fwa = lambda i: remote(xg.at[rows(p2, half, i)], xg.at[rows(p2, half, i)], fw_s.at[i], fw_r.at[i], pts=p1)
    fwb = lambda i: remote(xg.at[rows(p2, 1 - half, i)], xg.at[rows(p2, 1 - half, i)], fw_s.at[8 + i], fw_r.at[8 + i], pts=p1)
    qrow = lambda o: pl.ds(2 * o, 2)
    qcp = [remote(q_in, qv.at[qrow(p)], qsend.at[a - 1], qrecv.at[a - 1], pts=flip(p, a)) for a in (1, 2, 3)]
    for c in qcp:
        c.start()
    for i in range(8):
        py(i).start()
    sib.start()
    st = [pltpu.make_async_copy(x_in.at[pl.ds(i * 1024, 1024)], (rb0, rb1)[i], xsem.at[i]) for i in range(2)]
    for c in st:
        c.start()
    mcp = pltpu.make_async_copy(mu_in.at[pl.ds(pl.multiple_of(p * kd, kd), kd)], S, osem.at[0])
    mcp.start()
    lcp = pltpu.make_async_copy(lw_in, lw_b, osem.at[1])
    lcp.start()
    qv[qrow(p)] = q_in[...]
    for i, c in enumerate(st):
        c.wait()
        st[i] = pltpu.make_async_copy((rb0, rb1)[i], xg.at[pl.ds(pl.multiple_of(p * 2048 + i * 1024, 1024), 1024)], xsem.at[i])
        st[i].start()
    mcp.wait()
    lcp.wait()
    for c in st:
        c.wait()
    for c in qcp:
        c.wait()

    rest = pl.ds(FAR, kd - FAR)
    mid = (kd - FAR) // 2
    bulk = lambda i: remote(mub.at[pl.ds(FAR + i * mid, mid)], mub2.at[pl.ds(i * mid, mid)], b_s.at[i], b_r.at[i], pts=p2)
    bulk_rows = lambda: remote(row1, row2, b_s.at[2], b_r.at[2], pts=p2)

    def as_row(ref, g):
        blk = ref[g * 128:(g + 1) * 128, :]
        eye = lax.broadcasted_iota(jnp.int32, (128, 128), 0) == lax.broadcasted_iota(jnp.int32, (128, 128), 1)
        return jnp.sum(jnp.where(eye, blk, 0.0), axis=0, keepdims=True)

    def take_py(i):
        py(i).wait_recv()
        pz(i).start()
        fwa(i).start()

    def take_pz(i):
        pz(i).wait_recv()
        fwb(i).start()

    def arrive(n):
        if n == 2:
            sib.wait_recv()
            take_py(0)
        elif n == 3:
            take_py(1)
        elif n == 4:
            take_pz(0)
            for i in range(2, 5):
                take_py(i)
                take_pz(i - 1)
        elif n == 6:
            for i in range(5, 8):
                take_py(i)
                take_pz(i - 1)
            take_pz(7)
        elif n in (5, 7):
            for i in range(4):
                fwa(i + 4 * (n == 7)).wait_recv()
                fwb(i + 4 * (n == 7)).wait_recv()

    def fetch(b, slot):
        o, h = b // 2, lax.rem(b, 2)
        return [pltpu.make_async_copy(xg.at[pl.ds(pl.multiple_of(o * 2048 + g * 1024 + h * STRIP, STRIP), STRIP)],
                                      xbuf.at[slot, pl.ds(g * STRIP, STRIP)], fsem.at[slot, g]) for g in range(2)]

    def start(cs):
        for c in cs:
            c.start()

    def wait(cs):
        for c in cs:
            c.wait()

    def sweep(t, _):
        par = lax.rem(t, 2)
        first_sweep = t == 0
        pe = jnp.where(first_sweep, p, 0)
        nb2 = -2.0 * beta[t]

        def order(k):
            r = 2 * (k // 4) + jnp.where(first_sweep, lax.rem(k, 2) * (k // 4) + (lax.rem(k, 4) // 2) * (1 - k // 4), lax.rem(k, 4) // 2)
            h = jnp.where(first_sweep, lax.rem(k, 2) * (1 - k // 4) + (lax.rem(k, 4) // 2) * (k // 4), lax.rem(k, 2))
            return 2 * flip(pe, r) + h

        start(fetch(order(0), 0))
        def load_means(g, _):
            r = pl.ds(pl.multiple_of(g * 64, 64), 64)
            v = S[r, :]
            mub[r, :] = v.astype(BF16)
            hmu_b[r, :] = jnp.broadcast_to(0.5 * jnp.sum(v * v, axis=1, keepdims=True), (64, 128))
            nacc[r, :] = jnp.zeros((64, 128), F32)
            return 0

        lax.fori_loop(0, kd // 64, load_means, 0)

        @pl.when(t == sweeps - 1)
        def _():
            for g in range(kd // 128):
                row1[0, g:g + 1, :] = as_row(hmu_b, g)
                row1[1, g:g + 1, :] = as_row(lw_b, g)
            bulk_rows().start()
            bulk(0).start()

        def send1(k):
            return [remote(own1.at[k], buf1.at[a - 1, k], s1s.at[a - 1, k], s1r.at[a - 1, k], comp=lax.rem(z + a, 4)) for a in (1, 2, 3)]

        def send2(b):
            return [remote(own2.at[b], buf2.at[par, a - 1, b], s2s.at[a - 1, b], s2r.at[par, a - 1, b], pts=flip(p, a)) for a in (1, 2, 3)]

        def merge(ms):
            m, s = [v[0:1] for v in ms], [v[1:2] for v in ms]
            top = jnp.maximum(jnp.maximum(m[0], m[1]), jnp.maximum(m[2], m[3]))
            return top, sum(si * jnp.exp(mi - top) for mi, si in zip(m, s))

        def publish(k):
            b = order(k)
            mm = jnp.max(mst[b], axis=0, keepdims=True)
            own1[k, 0:1] = mm
            own1[k, 1:2] = jnp.sum(sst[b] * jnp.exp(mst[b] - mm), axis=0, keepdims=True)
            start(send1(k))

        def relay(k):
            wait(send1(k))
            b = order(k)
            mm, ss = merge([own1[k]] + [buf1[a, k] for a in range(3)])
            own2[b, 0:1] = mm
            own2[b, 1:2] = ss
            start(send2(b))

        def settle(b):
            wait(send2(b))
            mm, ss = merge([own2[b]] + [buf2[par, a, b] for a in range(3)])
            l = mm + jnp.log(ss)
            lse[b] = l
            mst[b] = jnp.exp(mst[b] - l)

        def step_a(k, dst, src, slot, first, last, prepare):
            if not last:
                wait(fetch(order(k), slot))
                for cond, n in prepare:
                    @pl.when(jnp.logical_and(first_sweep, cond))
                    def _():
                        arrive(n)
                if prepare:
                    start(fetch(order(k + 1), 1 - slot))
            if not first:
                b = order(k - 1)
            for u in range(NB // 256):
                sl = slice(u * 256, (u + 1) * 256)
                if not last:
                    dst[:, sl] = lax.dot_general(mub[...], xbuf[slot, sl, :], (((1,), (1,)), ((), ())), preferred_element_type=F32)
                if not first:
                    for l0 in (u * 256, u * 256 + 128):
                        ln = slice(l0, l0 + 128)
                        q = jnp.broadcast_to(qv[b, :, ln], (CH, 128))
                        for c in range(kd // CH):
                            r = slice(c * CH, (c + 1) * CH)
                            lg = lw_b[r, :] + nb2 * ((hmu_b[r, :] - src[r, ln]) + q)
                            m = jnp.max(lg, axis=0, keepdims=True)
                            e = jnp.exp(lg - m)
                            pm[b, r, ln] = e
                            mst[b, c:c + 1, ln] = m
                            sst[b, c:c + 1, ln] = jnp.sum(e, axis=0, keepdims=True)
            if not first:
                publish(k - 1)

        yes = t >= 0
        step_a(0, ab0, ab1, 0, True, False, [(yes, 1)])

        def body_a(i, _):
            step_a(2 * i + 1, ab1, ab0, 1, False, False, [(i == 0, 2), (i == 1, 4), (i == 2, 6)])

            @pl.when(i > 0)
            def _():
                relay(2 * i - 2)
                relay(2 * i - 1)
            step_a(2 * i + 2, ab0, ab1, 0, False, False, [(i == 0, 3), (i == 1, 5), (i == 2, 7)])
            return 0

        lax.fori_loop(0, nblk // 2 - 1, body_a, 0)
        step_a(nblk - 1, ab1, ab0, 1, False, False, [])
        start(fetch(0, 0))
        relay(nblk - 4)
        relay(nblk - 3)
        step_a(nblk, ab0, ab1, 0, False, True, [])
        relay(nblk - 2)

        @pl.when(first_sweep)
        def _():
            relay(nblk - 1)

        S[...] = jnp.zeros_like(S)

        def step_s(j, rd, rs, slot, first, last):
            if not last:
                settle(j)
            if not first:
                wait(fetch(j - 1, slot))
                if not last:
                    start(fetch(j, 1 - slot))
            for u in range(4):
                if not last:
                    for r0 in range(u * (kd // 4), (u + 1) * (kd // 4), 16):
                        r = slice(r0, r0 + 16)
                        c = r0 // CH
                        rr = pm[j, r, :] * jnp.broadcast_to(mst[j, c:c + 1, :], (16, NB))
                        rd[r, :] = rr.astype(BF16)
                        acc = rr[:, 0:128]
                        for l0 in range(128, NB, 128):
                            acc += rr[:, l0:l0 + 128]
                        nacc[r, :] += acc
                if not first:
                    sl = slice(u * (d // 4), (u + 1) * (d // 4))
                    S[:, sl] += jnp.dot(rs[...], xbuf[slot, :, sl], preferred_element_type=F32)

        step_s(0, rb0, rb1, 1, True, False)

        def body_s(i, _):
            step_s(2 * i + 1, rb1, rb0, 0, False, False)

            @pl.when(jnp.logical_and(i == 0, t > 0))
            def _():
                relay(nblk - 1)

            @pl.when(jnp.logical_and(i == 0, t == sweeps - 1))
            def _():
                bulk(1).start()
            step_s(2 * i + 2, rb0, rb1, 1, False, False)
            return 0

        lax.fori_loop(0, nblk // 2 - 1, body_s, 0)
        step_s(nblk - 1, rb1, rb0, 0, False, False)
        step_s(nblk, rb0, rb1, 1, False, True)
        def finish(g, _):
            r = pl.ds(pl.multiple_of(g * 64, 64), 64)
            n = jnp.sum(nacc[r, :], axis=1, keepdims=True)
            S[r, :] = S[r, :] * (1.0 / (n + COUNT_EPS))
            lw = jnp.log((n + PRIOR_ALPHA) / (nblk * NB + 16 * kd * PRIOR_ALPHA))
            lw_b[r, :] = jnp.broadcast_to(lw, (64, 128))
            return 0

        lax.fori_loop(0, kd // 64, finish, 0)
        return 0

    lax.fori_loop(0, sweeps, sweep, 0)

    quarter = lambda o, r0, n: pl.ds(pl.multiple_of(o * kd + r0, 128), n)
    out_own = pltpu.make_async_copy(S, mu_out.at[quarter(p, 0, kd)], osem.at[0])
    out_sib = remote(S, mu_out.at[quarter(p, 0, kd)], o_s.at[0], o_r.at[0], pts=p1)
    out_far = [remote(S.at[pl.ds(i * 128, 128)], mu_out.at[quarter(p, i * 128, 128)], o_s.at[1 + i], o_r.at[1 + i], pts=p2) for i in range(FAR // 128)]
    out_fwd = [remote(mu_out.at[quarter(p2, i * 128, 128)], mu_out.at[quarter(p2, i * 128, 128)], o_s.at[4 + i], o_r.at[4 + i], pts=p1) for i in range(FAR // 128)]
    for g in range(kd // 128):
        lw_all[p, g:g + 1, :] = as_row(lw_b, g)
    out_lw = [remote(lw_all.at[p], lw_all.at[p], w_s.at[a - 1], w_r.at[a - 1], pts=flip(p, a)) for a in (1, 2, 3)]
    start(out_lw)
    start(out_far)
    out_own.start()
    out_sib.start()

    rn = kd - FAR
    S2 = pm.at[0]
    bulk_rows().wait()
    for i in range(2):
        bulk(i).wait()
    for g in range(rn // 128):
        for v, ref in ((0, hmu_b2), (1, lw_b2)):
            ref[g * 128:(g + 1) * 128, :] = jnp.broadcast_to(row2[v, FAR // 128 + g:FAR // 128 + g + 1, :], (128, 128)).T
    nb2 = -2.0 * beta[sweeps - 1]
    nacc[...] = jnp.zeros_like(nacc)
    S2[0:rn, :] = jnp.zeros((rn, d), F32)
    start(fetch(0, 0))

    def step_d(j, dst, src, rb, first, last):
        now, before = lax.rem(j, 3), lax.rem(j + 2, 3)
        if not last:
            wait(fetch(j, now))

            @pl.when(j + 1 < nblk)
            def _():
                start(fetch(j + 1, lax.rem(j + 1, 3)))
        for u in range(4):
            if not last:
                sl = slice(u * (NB // 4), (u + 1) * (NB // 4))
                dst[0:rn, sl] = lax.dot_general(mub2[...], xbuf[now, sl, :], (((1,), (1,)), ((), ())), preferred_element_type=F32)
            if not first:
                for r0 in range(u * (rn // 4), (u + 1) * (rn // 4), 16):
                    r = slice(r0, r0 + 16)
                    wide = lambda ref: jnp.concatenate([ref[r, :]] * (NB // 128), axis=1)
                    spread = lambda v: jnp.broadcast_to(v, (16, NB))
                    lg = wide(lw_b2) + nb2 * ((wide(hmu_b2) - src[r, :]) + spread(qv[j - 1]))
                    rr = jnp.exp(lg - spread(lse[j - 1]))
                    rb[r, :] = rr.astype(BF16)
                    acc = rr[:, 0:128]
                    for l0 in range(128, NB, 128):
                        acc += rr[:, l0:l0 + 128]
                    nacc[r, :] += acc
        if not first:
            for u in range(4):
                sl = slice(u * (d // 4), (u + 1) * (d // 4))
                S2[0:rn, sl] += jnp.dot(rb[0:rn, :], xbuf[before, :, sl], preferred_element_type=F32)

    step_d(0, ab0, ab1, rb0, True, False)

    def body_d(i, _):
        step_d(2 * i + 1, ab1, ab0, rb0, False, False)
        step_d(2 * i + 2, ab0, ab1, rb1, False, False)
        return 0

    lax.fori_loop(0, nblk // 2 - 1, body_d, 0)
    step_d(nblk - 1, ab1, ab0, rb0, False, False)
    step_d(nblk, ab0, ab1, rb1, False, True)

    def finish2(g, _):
        r = pl.ds(pl.multiple_of(g * 64, 64), 64)
        n2 = jnp.sum(nacc[r, :], axis=1, keepdims=True)
        S2[r, :] = S2[r, :] * (1.0 / (n2 + COUNT_EPS))
        return 0

    lax.fori_loop(0, rn // 64, finish2, 0)
    src2 = S2.at[pl.ds(0, rn)]
    out_dup = pltpu.make_async_copy(src2, mu_out.at[quarter(p2, FAR, rn)], osem.at[1])
    out_dsib = remote(src2, mu_out.at[quarter(p2, FAR, rn)], o_s.at[7], o_r.at[7], pts=p1)
    out_dsib.start()
    out_dup.start()
    for c, f in zip(out_far, out_fwd):
        c.wait()
        f.start()
    sib.wait_send()
    for i in range(8):
        py(i).wait_send()
        pz(i).wait_send()
        fwa(i).wait_send()
        fwb(i).wait_send()
    wait(out_lw)
    lw_out[...] = lw_all[...]
    lse_out[...] = lse[qrow(p)]
    out_own.wait()
    out_sib.wait()
    wait(out_fwd)
    out_dup.wait()
    out_dsib.wait()


def solution(mesh):
    def per_device(points, mean_vecs, log_w, inv_temp):
        n_loc, d = points.shape
        k_loc = mean_vecs.shape[0]
        kd = k_loc // mesh.shape["pts"]
        nblk = n_loc * mesh.shape["pts"] // NB
        p = lax.axis_index("pts")
        x_sq = 0.5 * jnp.sum(jnp.square(points.astype(F32)), axis=1)
        q_in = x_sq.reshape(2, 2, STRIP).transpose(1, 0, 2).reshape(2, 1, NB)
        lw_in = jnp.broadcast_to(lax.dynamic_slice(log_w, (p * kd,), (kd,))[:, None], (kd, 128))
        V, D = pltpu.VMEM, pltpu.SemaphoreType.DMA
        bs = lambda m: pl.BlockSpec(memory_space=m)
        means, logw, lse, _ = pl.pallas_call(
            em_kernel,
            out_shape=(
                jax.ShapeDtypeStruct((k_loc, d), F32),
                jax.ShapeDtypeStruct((k_loc // kd, kd // 128, 128), F32),
                jax.ShapeDtypeStruct((2, 1, NB), F32),
                jax.ShapeDtypeStruct((nblk * NB, d), BF16),
            ),
            in_specs=[bs(pltpu.SMEM), bs(pl.ANY), bs(pl.ANY), bs(pl.ANY), bs(V)],
            out_specs=(bs(pl.ANY), bs(V), bs(V), bs(pl.ANY)),
            scratch_shapes=[
                V((nblk, kd, NB), F32), V((3, NB, d), BF16), V((kd, d), BF16),
                V((kd, NB), F32), V((kd, NB), F32), V((kd, NB), BF16), V((kd, NB), BF16),
                V((kd, d), F32), V((kd, 128), F32), V((kd, 128), F32), V((kd, 128), F32),
                V((nblk, kd // CH, NB), F32), V((nblk, kd // CH, NB), F32),
                V((nblk, 1, NB), F32), V((nblk, 1, NB), F32),
                V((nblk, 2, NB), F32), V((3, nblk, 2, NB), F32),
                V((nblk, 2, NB), F32), V((2, 3, nblk, 2, NB), F32),
                V((kd - FAR, d), BF16), V((kd - FAR, 128), F32), V((kd - FAR, 128), F32),
                V((2, kd // 128, 128), F32), V((2, kd // 128, 128), F32), V((k_loc // kd, kd // 128, 128), F32),
                D((3, 2)), D((2,)), D((3,)), D((3,)),
                D((3, nblk)), D((3, nblk)), D((3, nblk)), D((2, 3, nblk)),
                D, D, D((8,)), D((8,)), D((8,)), D((8,)), D((16,)), D((16,)),
                D((3,)), D((3,)), D((3,)), D((3,)), D((8,)), D((8,)), D((2,)),
            ],
            compiler_params=pltpu.CompilerParams(
                collective_id=0, has_side_effects=True, vmem_limit_bytes=67043328),
            name="em_sweeps",
        )(inv_temp, points, mean_vecs, lw_in, q_in)
        lse_rows = lse.reshape(2, 2, STRIP).transpose(1, 0, 2).reshape(n_loc)
        return means, logw.reshape(k_loc), lse_rows

    comp_spec, row_spec = P(("fit", "comp")), P(("fit", "pts"))
    return jax.shard_map(
        per_device,
        mesh=mesh,
        in_specs=(P(("fit", "pts"), None), P(("fit", "comp"), None), comp_spec, P()),
        out_specs=(P(("fit", "comp"), None), comp_spec, row_spec),
        check_vma=False,
    )
```
